256 devices in a mesh: group: 2 (over y), ctx: 32 (over z, core), exp: 4 (over x).
Axes of the slice: x: 4, y: 2, z: 16, core: 2. Of those that a mesh axis runs over, the one named last changes fastest.
The devices are a block of a 4x16x16 slice.
Arguments:
- queries: bfloat16 [4096, 4096], P(('group', 'ctx'), 'exp'), parts along dimension 0, may hold values from -6 to 6
- new_keys: bfloat16 [4096, 1024], P(('group', 'ctx'), 'exp'), parts along dimension 0, may hold values from -6 to 6
- new_values: bfloat16 [4096, 1024], P(('group', 'ctx'), 'exp'), parts along dimension 0, may hold values from -6 to 6
- cache_keys: bfloat16 [16384, 1024], P(('group', 'ctx'), 'exp'), parts along dimension 0, may hold values from -6 to 6
- cache_values: bfloat16 [16384, 1024], P(('group', 'ctx'), 'exp'), parts along dimension 0, may hold values from -6 to 6
- offset: int32 [2], P('group'), parts along dimension 0, may hold values from 4096 to 8192
- token_ids: int32 [4096], P(('group', 'ctx')), parts along dimension 0, may hold values from 0 to 128255, as said below
- expert_table: int32 [256512], P('group'), parts along dimension 0, may hold values from 0 to 3
- norm_gain: float32 [4096], replicated, may hold values from 0.5 to 1.5
- w_gate: bfloat16 [4, 4096, 14336], P('exp', None, 'ctx'), may hold values from -0.09375 to 0.09375
- w_up: bfloat16 [4, 4096, 14336], P('exp', None, 'ctx'), may hold values from -0.09375 to 0.09375
- w_down: bfloat16 [4, 14336, 4096], P('exp', 'ctx'), may hold values from -0.046875 to 0.046875
Outputs:
- mixed: bfloat16 [4096, 4096], P(('group', 'ctx'), 'exp'), parts along dimension 0
The draws below stay inside these ranges and needn't reach their ends.
There are 2 independent parts, one for each index of `group`. The reference program is written for one: setup_inputs(seed, part) draws one part's arguments, and reference() takes and returns one part's arrays. A program takes and returns all parts, laid end to end along the dimension named above; an argument that names none is the same for every part. Nothing has to cross between parts.
Inputs may be any that keep to these rules, and one draw needn't show every extreme that they name: Cache positions at or beyond offset are not yet filled. `token_ids`: in every block of 64 consecutive stretch tokens (one block per index of ctx) at most 32 tokens map to one expert through expert_table, and one expert takes exactly 32 tokens of every block.
All inputs are finite; a program needn't handle non-finite values.
Results may differ from the reference program's by a relative error of at most 0.025.
Values may be sent and summed in bfloat16 or wider, within the bound.
A program may use at most 128 MiB of HBM per device.

```python
import math
import jax
import jax.numpy as jnp
from jax import lax

HEADS = 32
KV_HEADS = 8
HEAD_DIM = 128
VOCAB = 128256
FF_DEV = 448
Q_DEV = 64
D = 4096
CAP = 32
STRETCH = 2048
CACHE = 8192
EXPERTS = 4
FF = 14336
N_CTX = 32


def drawn_field(key, shape):
    return jnp.clip(jax.random.normal(key, shape, jnp.float32), -6.0, 6.0)


def draw_queries(key, part):
    drawn = drawn_field(jax.random.fold_in(key, 3), (STRETCH, HEADS, HEAD_DIM))
    return drawn.reshape(STRETCH, HEADS * HEAD_DIM).astype(jnp.bfloat16)


def draw_cache_keys(key, part):
    drawn = drawn_field(jax.random.fold_in(key, 4), (CACHE, KV_HEADS, HEAD_DIM))
    return drawn.reshape(CACHE, KV_HEADS * HEAD_DIM).astype(jnp.bfloat16)


def routing_pair(key):
    base = jax.random.fold_in(key, 29)
    table_key, hot_key, rest_key, order_key, pick_key = jax.random.split(base, 5)
    table = jax.random.randint(table_key, (VOCAB,), 0, EXPERTS).astype(jnp.int32)
    table = table.at[:EXPERTS].set(jnp.arange(EXPERTS, dtype=jnp.int32))
    favored = jax.random.randint(hot_key, (), 0, EXPERTS).astype(jnp.int32)
    others = (favored + jax.random.randint(rest_key, (N_CTX, Q_DEV - CAP), 1, EXPERTS)) % EXPERTS
    labels = jnp.concatenate([jnp.full((N_CTX, CAP), favored, jnp.int32), others.astype(jnp.int32)], axis=1)
    orders = jax.vmap(lambda sub_key: jax.random.permutation(sub_key, Q_DEV))(jax.random.split(order_key, N_CTX))
    labels = jnp.take_along_axis(labels, orders, axis=1).reshape(STRETCH)
    candidates = jax.random.randint(pick_key, (STRETCH, 64), EXPERTS, VOCAB).astype(jnp.int32)
    matches = table[candidates] == labels[:, None]
    first = jnp.argmax(matches, axis=1)
    found = jnp.any(matches, axis=1)
    picked_ids = jnp.take_along_axis(candidates, first[:, None], axis=1)[:, 0]
    token_list = jnp.where(found, picked_ids, labels).astype(jnp.int32)
    return (table, token_list)


def draw_token_ids(key, part):
    return routing_pair(key)[1]


def draw_expert_table(key, part):
    return routing_pair(key)[0]


def block_scale(rng, dims, cuts, low, high):
    def one(axis_at, parts):
        draws = jax.random.uniform(jax.random.fold_in(jax.random.fold_in(rng, 6), axis_at), (parts,), jnp.float32, low / len(cuts), high / len(cuts))
        return jnp.repeat(jnp.exp(draws), dims[axis_at] // parts).reshape((-1,) + (1,) * (len(dims) - axis_at - 1))

    gain = one(*cuts[0])
    for cut in cuts[1:]:
        gain = gain * one(*cut)
    return gain


def noise(key, dims, spread, bound, cuts=(), kind=jnp.bfloat16):
    entries = spread * jax.random.normal(key, dims, jnp.float32)
    if cuts:
        entries = entries * block_scale(key, dims, cuts, -0.22, 0.18)
    return jnp.clip(entries, -bound, bound).astype(kind)


def setup_inputs(seed: int = 0, part: int = 0) -> dict:
    seeds = jax.random.split(jax.random.key(seed), 13)
    part_keys = jax.random.split(jax.random.fold_in(seeds[12], part), 13)
    queries = draw_queries(jax.random.fold_in(jax.random.fold_in(seeds[12], part), 71), part)
    new_keys = noise(part_keys[1], (STRETCH, KV_HEADS * HEAD_DIM), 1.0, 6.0, ((0, 32), (1, 4)))
    new_values = noise(part_keys[2], (STRETCH, KV_HEADS * HEAD_DIM), 1.0, 6.0, ((0, 32), (1, 4)))
    cache_keys = draw_cache_keys(jax.random.fold_in(jax.random.fold_in(seeds[12], part), 71), part)
    cache_values = noise(part_keys[4], (CACHE, KV_HEADS * HEAD_DIM), 1.0, 6.0, ((0, 32), (1, 4)))
    offset = jax.random.randint(part_keys[5], (1,), CACHE // 2, CACHE + 1).astype(jnp.int32)
    token_ids = draw_token_ids(jax.random.fold_in(jax.random.fold_in(seeds[12], part), 71), part)
    expert_table = draw_expert_table(jax.random.fold_in(jax.random.fold_in(seeds[12], part), 71), part)
    norm_gain = jnp.clip(1.0 + 0.1 * jax.random.normal(seeds[8], (D,), jnp.float32), 0.5, 1.5)
    w_gate = noise(seeds[9], (EXPERTS, D, FF), D ** -0.5, 0.09375, ((0, 4), (2, 32)))
    w_up = noise(seeds[10], (EXPERTS, D, FF), D ** -0.5, 0.09375, ((0, 4), (2, 32)))
    w_down = noise(seeds[11], (EXPERTS, FF, D), FF ** -0.5, 0.046875, ((0, 4), (1, 32)))
    return dict(queries=queries, new_keys=new_keys, new_values=new_values, cache_keys=cache_keys, cache_values=cache_values, offset=offset, token_ids=token_ids, expert_table=expert_table, norm_gain=norm_gain, w_gate=w_gate, w_up=w_up, w_down=w_down)


def reference(queries, new_keys, new_values, cache_keys, cache_values, offset, token_ids, expert_table, norm_gain, w_gate, w_up, w_down):
    group = HEADS // KV_HEADS
    total_keys = CACHE + STRETCH
    grouped = queries.astype(jnp.float32).reshape(STRETCH, KV_HEADS, group, HEAD_DIM)
    key_rows = jnp.concatenate([cache_keys, new_keys], axis=0).astype(jnp.float32).reshape(total_keys, KV_HEADS, HEAD_DIM)
    value_rows = jnp.concatenate([cache_values, new_values], axis=0).astype(jnp.float32).reshape(total_keys, KV_HEADS, HEAD_DIM)
    stretch_index = jnp.arange(STRETCH, dtype=jnp.int32)
    cache_ok = jnp.arange(CACHE, dtype=jnp.int32) < offset[0]
    allowed = jnp.concatenate([jnp.broadcast_to(cache_ok[None, :], (STRETCH, CACHE)), stretch_index[None, :] <= stretch_index[:, None]], axis=1)

    def per_head(head):
        query_head = lax.dynamic_index_in_dim(grouped, head, 1, keepdims=False)
        key_head = lax.dynamic_index_in_dim(key_rows, head, 1, keepdims=False)
        value_head = lax.dynamic_index_in_dim(value_rows, head, 1, keepdims=False)
        scores = jnp.einsum('tgd,sd->tgs', query_head, key_head) * (1.0 / math.sqrt(HEAD_DIM))
        usable = allowed[:, None, :]
        peak = lax.optimization_barrier(jnp.max(jnp.where(usable, scores, -1e+30), axis=-1))
        unnorm = jnp.where(usable, jnp.exp(scores - peak[..., None]), 0.0)
        total = lax.optimization_barrier(jnp.sum(unnorm, axis=-1))
        rounded = lax.optimization_barrier(unnorm.astype(jnp.bfloat16)).astype(jnp.float32)
        numer = jnp.einsum('tgs,sd->tgd', rounded, value_head)
        return numer / total[..., None]
    heads_out = lax.map(per_head, jnp.arange(KV_HEADS, dtype=jnp.int32))
    attended = jnp.transpose(heads_out, (1, 0, 2, 3)).reshape(STRETCH, D).astype(jnp.bfloat16)
    chosen = expert_table[token_ids]
    blocks = chosen.reshape(N_CTX, Q_DEV)
    onehot = (blocks[..., None] == jnp.arange(EXPERTS, dtype=jnp.int32)).astype(jnp.int32)
    earlier = jnp.cumsum(onehot, axis=1) - onehot
    slot = lax.optimization_barrier(jnp.sum(earlier * onehot, axis=-1))
    row_of = (jnp.arange(N_CTX, dtype=jnp.int32)[:, None] * CAP + slot).reshape(STRETCH).astype(jnp.int32)
    values32 = attended.astype(jnp.float32)
    scale = lax.rsqrt(lax.optimization_barrier(jnp.mean(values32 * values32, axis=-1, keepdims=True)) + 1e-05)
    normed = (values32 * scale * norm_gain).astype(jnp.bfloat16)

    def per_expert(carry, which):
        select = chosen == which
        place = jnp.where(select, row_of, N_CTX * CAP).astype(jnp.int32)
        buffer = jnp.zeros((N_CTX * CAP, D), jnp.bfloat16).at[place].set(normed, mode='drop')
        gate_w = lax.dynamic_index_in_dim(w_gate, which, 0, keepdims=False)
        up_w = lax.dynamic_index_in_dim(w_up, which, 0, keepdims=False)
        down_w = lax.dynamic_index_in_dim(w_down, which, 0, keepdims=False)
        gate = jnp.dot(buffer, gate_w, preferred_element_type=jnp.float32)
        upper = jnp.dot(buffer, up_w, preferred_element_type=jnp.float32)
        hidden = (jax.nn.silu(gate) * upper).astype(jnp.bfloat16)

        def add_slice(acc, piece):
            start = (piece * FF_DEV).astype(jnp.int32)
            part_h = lax.dynamic_slice_in_dim(hidden, start, FF_DEV, 1)
            part_w = lax.dynamic_slice_in_dim(down_w, start, FF_DEV, 0)
            partial_sum = jnp.dot(part_h, part_w, preferred_element_type=jnp.float32)
            partial_sum = lax.optimization_barrier(partial_sum.astype(jnp.bfloat16)).astype(jnp.float32)
            return (acc + partial_sum, None)
        summed, _ = lax.scan(add_slice, jnp.zeros((N_CTX * CAP, D), jnp.float32), jnp.arange(N_CTX, dtype=jnp.int32))
        picked = summed[jnp.clip(row_of, 0, N_CTX * CAP - 1)]
        return (carry + jnp.where(select[:, None], picked, 0.0), None)
    expert_out, _ = lax.scan(per_expert, jnp.zeros((STRETCH, D), jnp.float32), jnp.arange(EXPERTS, dtype=jnp.int32))
    return (normed.astype(jnp.float32) + expert_out).astype(jnp.bfloat16)
```

```python
import functools
import math

import jax
import jax.numpy as jnp
from jax import lax
from jax.experimental import pallas as pl
from jax.experimental.pallas import tpu as pltpu
from jax.sharding import PartitionSpec as P

MESH = pl.DeviceIdType.MESH
F32 = jnp.float32
BF16 = jnp.bfloat16
HEAD = 128
NEG = -1e30
VMEM_LIMIT = 64000 * 1024


def layer_kernel(
    nz,
    nx,
    offset_ref,
    q_hbm,
    nk_hbm,
    nv_hbm,
    ck_hbm,
    cv_hbm,
    disp_hbm,
    coll_ref,
    gain_ref,
    wg_hbm,
    wu_hbm,
    wd_hbm,
    out_ref,
    kbuf,
    vbuf,
    qbuf,
    qcat,
    dbuf,
    tok_ref,
    m_ref,
    l_ref,
    o_ref,
    att,
    packed,
    arr,
    rows,
    sums,
    rsb,
    gate_s,
    hid,
    comb,
    ret,
    wg,
    wu,
    wd,
    loc_sem,
    pair_send,
    pair_recv,
    w_loc,
    w_send,
    w_recv,
    kv_send,
    kv_recv,
    a_send,
    a_recv,
    g_send,
    g_recv,
    r_send,
    r_recv,
    b_send,
    b_recv,
):
    ctx = lax.axis_index("ctx")
    x = lax.axis_index("exp")
    z = ctx // 2
    c = ctx % 2
    oc = 1 - c
    half = nz // 2
    right = {"ctx": ((z + 1) % nz) * 2 + c, "exp": x}
    left = {"ctx": ((z + nz - 1) % nz) * 2 + c, "exp": x}
    ahead = (right, left)
    pair = {"ctx": z * 2 + oc, "exp": x}
    T = q_hbm.shape[0]
    CK = ck_hbm.shape[0]
    NK = nk_hbm.shape[0]
    QW = qbuf.shape[2]
    group = QW // HEAD
    cap = arr.shape[0]
    width = arr.shape[1]
    hrow = cap // 2
    hcol = width // 2

    def remote(src, dst, ssem, rsem, dev):
        return pltpu.make_async_remote_copy(
            src_ref=src, dst_ref=dst, send_sem=ssem, recv_sem=rsem, device_id=dev, device_id_type=MESH
        )

    kcol = pl.ds(pl.multiple_of(c * HEAD, HEAD), HEAD)
    kcol_o = pl.ds(pl.multiple_of(oc * HEAD, HEAD), HEAD)
    qcol = pl.ds(pl.multiple_of(c * QW, HEAD), QW)
    qcol_o = pl.ds(pl.multiple_of(oc * QW, HEAD), QW)
    parts = (
        (ck_hbm, kbuf, 0, CK),
        (nk_hbm, kbuf, CK, NK),
        (cv_hbm, vbuf, 0, CK),
        (nv_hbm, vbuf, CK, NK),
    )
    local = []
    for i, (src, buf, lo, n) in enumerate(parts):
        local.append(
            pltpu.make_async_copy(src.at[:, kcol], buf.at[0, 0, pl.ds(lo, n), :], loc_sem.at[i])
        )
    local.append(pltpu.make_async_copy(q_hbm.at[:, qcol], qbuf.at[0], loc_sem.at[4]))
    local.append(pltpu.make_async_copy(disp_hbm, dbuf.at[0], loc_sem.at[5]))
    for cp in local:
        cp.start()

    barrier = pltpu.get_barrier_semaphore()
    others = []
    for d in range(nx):
        for k in range(2):
            if d or k:
                others.append((d, k))
    for dev in ahead:
        pl.semaphore_signal(barrier, inc=1, device_id=dev, device_id_type=MESH)
    for d, k in others:
        pl.semaphore_signal(
            barrier,
            inc=1,
            device_id={"ctx": z * 2 + (c + k) % 2, "exp": (x + d) % nx},
            device_id_type=MESH,
        )
    pl.semaphore_wait(barrier, 2 + len(others))

    swap = []
    for i, (src, buf, lo, n) in enumerate(parts):
        swap.append(
            remote(src.at[:, kcol_o], buf.at[0, 1, pl.ds(lo, n), :], pair_send.at[i], pair_recv.at[i], pair)
        )
    swap.append(remote(q_hbm.at[:, qcol_o], qbuf.at[1], pair_send.at[4], pair_recv.at[4], pair))
    swap.append(remote(disp_hbm, dbuf.at[1], pair_send.at[5], pair_recv.at[5], pair))
    for cp in swap:
        cp.start()

    def last_pos(d, s):
        return 2 * s - 1 if d == 0 else 2 * s - s // half

    def kv_chunk(k, pos):
        return (kbuf, vbuf)[k % 2].at[pos, k // 2]

    def kv_copy(d, k, s, pos):
        return remote(
            kv_chunk(k, pos),
            kv_chunk(k, last_pos(d, s)),
            kv_send.at[d, k],
            kv_recv.at[d, s - 1, k],
            ahead[d],
        )

    for i in range(4):
        local[i].wait()
    for k in (0, 1):
        for d in (0, 1):
            kv_copy(d, k, 1, 0).start()
    local[4].wait()
    local[5].wait()
    for i in range(4):
        swap[i].wait_recv()
    for k in (2, 3):
        for d in (0, 1):
            kv_copy(d, k, 1, 0).start()

    weights = ((wg_hbm, wg), (wu_hbm, wu), (wd_hbm, wd))
    w_own = [pltpu.make_async_copy(src.at[0], dst.at[0], w_loc.at[i]) for i, (src, dst) in enumerate(weights)]
    w_swap = [remote(src.at[0], dst.at[1], w_send.at[i], w_recv.at[i], pair) for i, (src, dst) in enumerate(weights)]
    for cp in w_own:
        cp.start()
    for cp in w_swap:
        cp.start()

    swap[4].wait_recv()
    swap[5].wait_recv()
    for g in range(group):
        for s in range(2):
            qcat[pl.ds((g * 2 + s) * T, T), :] = qbuf[s, :, pl.ds(g * HEAD, HEAD)]
    lanes = 2 * T * group
    lane = lax.broadcasted_iota(jnp.int32, (1, lanes), 1)
    bits = T.bit_length() - 1
    second = lax.shift_right_logical(lane, bits) & 1
    tok_ref[...] = z * (2 * T) + (lane & (T - 1)) + jnp.where(second == 0, c, oc) * T
    m_ref[...] = jnp.full_like(m_ref, NEG)
    l_ref[...] = jnp.zeros_like(l_ref)
    o_ref[...] = jnp.zeros_like(o_ref)
    scale = 1.0 / math.sqrt(HEAD)
    nt = (((1,), (1,)), ((), ()))
    tn = (((0,), (0,)), ((), ()))

    def attend(pos, src, zz):
        owner = zz * 2 + (c if src == 0 else oc)
        s = lax.dot_general(kbuf[pos, src], qcat[...], nt, preferred_element_type=F32) * scale
        crow = lax.broadcasted_iota(jnp.int32, (CK, 1), 0) + owner * CK
        sc = jnp.where(crow < offset_ref[0], s[:CK], NEG)
        nrow = lax.broadcasted_iota(jnp.int32, (NK, lanes), 0) + owner * NK
        sn = jnp.where(nrow <= tok_ref[...], s[CK:], NEG)
        m_old = m_ref[...]
        m_new = jnp.maximum(
            m_old,
            jnp.maximum(jnp.max(sc, axis=0, keepdims=True), jnp.max(sn, axis=0, keepdims=True)),
        )
        pc = jnp.exp(sc - m_new)
        pn = jnp.exp(sn - m_new)
        fade = jnp.exp(m_old - m_new)
        m_ref[...] = m_new
        l_ref[...] = (
            l_ref[...] * fade + jnp.sum(pc, axis=0, keepdims=True) + jnp.sum(pn, axis=0, keepdims=True)
        )
        p = jnp.concatenate([pc.astype(BF16), pn.astype(BF16)], axis=0)
        o_ref[...] = o_ref[...] * fade + lax.dot_general(vbuf[pos, src], p, tn, preferred_element_type=F32)

    def kv_step(s, carry):
        for k in range(4):
            for d in (0, 1):
                here = last_pos(d, s)
                kv_copy(d, k, s, here).wait_recv()
                onward = kv_copy(d, k, s + 1, here)
                if k // 2 == d:
                    onward.wait_send()
                    onward.start()
                else:

                    @pl.when(s < half - 1)
                    def _():
                        onward.wait_send()
                        onward.start()

            if k < 2:

                @pl.when(s > 1)
                def _():
                    attend(2 * s - 3, k, (z + nz - s + 1) % nz)

            else:
                attend(2 * s - 2, k - 2, (z + s - 1) % nz)
        return carry

    lax.fori_loop(1, half, kv_step, 0)
    for k in range(2):
        attend(2 * half - 3, k, (z + nz - half + 1) % nz)
    for k in range(2):
        attend(2 * half - 2, k, (z + half - 1) % nz)
    for d in (0, 1):
        for k in (2 * d, 2 * d + 1):
            kv_copy(d, k, half, 2 * half - 1).wait_recv()
        attend(2 * half - 1, d, (z + half) % nz)
    for k in range(4):
        for d in (0, 1):
            kv_copy(d, k, half, 0).wait_send()
    for cp in swap:
        cp.wait_send()

    done = o_ref[...] / l_ref[...]
    for g in range(group):
        att[:, pl.ds(g * HEAD, HEAD)] = done[:, g * 2 * T : (g + 1) * 2 * T].T.astype(BF16)
    for k in range(2):
        packed[k] = jnp.dot(
            dbuf[k, :, pl.ds(0, T)], att[pl.ds(k * T, T), :], preferred_element_type=F32
        ).astype(BF16)

    mine = pl.ds(pl.multiple_of((x * 2 + c) * QW, HEAD), QW)

    def slots(e):
        return pl.ds(pl.multiple_of(e * cap, cap), cap)

    there = []
    for d, k in others:
        e = (x + d) % nx
        there.append(
            remote(
                packed.at[k, slots(e), :],
                arr.at[:, mine],
                a_send.at[d, k],
                a_recv.at[d, k],
                {"ctx": z * 2 + (c + k) % 2, "exp": e},
            )
        )
    for cp in there:
        cp.start()
    arr[:, mine] = packed[0, slots(x), :]
    for cp in there:
        cp.wait_recv()
    v32 = arr[...].astype(F32)
    norm = lax.rsqrt(jnp.mean(v32 * v32, axis=-1, keepdims=True) + 1e-05)
    rows[pl.ds(0, cap), :] = (v32 * norm * gain_ref[...]).astype(BF16)

    def part(ref, pos, k):
        return ref.at[
            pl.ds(pl.multiple_of(pos * cap + (k // 2) * hrow, hrow), hrow), pl.ds((k % 2) * hcol, hcol)
        ]

    def row_copy(d, k, s, pos):
        return remote(
            part(rows, pos, k),
            part(rows, last_pos(d, s), k),
            g_send.at[d, k],
            g_recv.at[d, s - 1, k],
            ahead[d],
        )

    for k in range(4):
        for d in (0, 1):
            row_copy(d, k, 1, 0).start()
    for cp in there:
        cp.wait_send()
    for cp in w_own:
        cp.wait()
    for cp in w_swap:
        cp.wait()

    M = 4 * cap
    ncols = 4
    ncol = width // ncols

    def dense(g, i):
        lo = pl.multiple_of(g * M, M)
        if i < 4:
            src = i // 2
            w = (wg, wu)[i % 2]
            v = jnp.dot(rows[pl.ds(lo, M), :], w[src], preferred_element_type=F32)
            if i % 2 == 0:
                gate_s[...] = v
            else:
                g32 = gate_s[...]
                hid[src] = (g32 / (1.0 + jnp.exp(-g32)) * v).astype(BF16)
        else:
            cols = pl.ds((i - 4) * ncol, ncol)
            sums[pl.ds(lo, M), cols] = (
                jnp.dot(hid[0], wd[0, :, cols], preferred_element_type=F32)
                + jnp.dot(hid[1], wd[1, :, cols], preferred_element_type=F32)
            ).astype(BF16)

    pairs = half // 2

    def row_pair(j, carry):
        more = j < pairs - 1
        for o in range(2):
            s = 2 * j + 1 + o
            for k in range(4):
                for d in (0, 1):
                    here = last_pos(d, s)
                    arrive = row_copy(d, k, s, here)
                    onward = row_copy(d, k, s + 1, here)
                    keep = k // 2 == d

                    def on():
                        onward.wait_send()
                        onward.start()

                    if o == 0:
                        arrive.wait_recv()
                        if keep:
                            on()
                        else:
                            pl.when(more)(on)
                    elif keep:
                        arrive.wait_recv()
                        pl.when(more)(on)
                    else:

                        @pl.when(more)
                        def _():
                            arrive.wait_recv()
                            on()

                @pl.when(j > 0)
                def _():
                    dense(j - 1, o * 4 + k)

        return carry

    lax.fori_loop(0, pairs, row_pair, 0)
    for k in range(4):
        for d in (0, 1):
            row_copy(d, k, half, 0).wait_send()

    def sum_copy(d, k, s):
        pos = 2 * s - s // half if d == 0 else 2 * s - 1
        return remote(
            part(sums, pos, k),
            part(rsb.at[d], s - 1, k),
            r_send.at[d, k],
            r_recv.at[d, s - 1, k],
            ahead[d],
        )

    for i in range(8):
        dense(pairs - 1, i)
    for q in range(2):
        for d in (0, 1):
            sum_copy(d, 2 * d + q, half).start()

    def add_in(d, k, s):
        pos = 2 * s if d == 0 else 2 * s - 1
        sum_copy(d, k, s + 1).wait_recv()
        own = part(sums, pos, k)
        own[...] = (own[...].astype(F32) + part(rsb.at[d], s, k)[...].astype(F32)).astype(BF16)

    def sum_step(t, carry):
        s = half - 1 - t
        for q in range(2):
            for d in (0, 1):
                k = 2 * (1 - d) + q

                @pl.when(t > 0)
                def _():
                    add_in(d, k, s)
                    sum_copy(d, k, s).wait_send()

                sum_copy(d, k, s).start()
        for q in range(2):
            for d in (0, 1):
                k = 2 * d + q
                add_in(d, k, s)
                sum_copy(d, k, s).wait_send()
                sum_copy(d, k, s).start()
        return carry

    lax.fori_loop(0, half - 1, sum_step, 0)

    for h in range(2):
        for q in range(2):
            k = 2 * h + q
            for d in (0, 1):
                sum_copy(d, k, 1).wait_recv()
            total = part(rows, 0, k)[...].astype(F32) + (
                part(sums, 0, k)[...].astype(F32)
                + part(rsb.at[0], 0, k)[...].astype(F32)
                + part(rsb.at[1], 0, k)[...].astype(F32)
            )
            part(comb, 0, k)[...] = total.astype(BF16)
    tw = width // nx

    def cols_of(e):
        return pl.ds(pl.multiple_of(e * tw, HEAD), tw)

    back = []
    for d in range(1, nx):
        e = (x + d) % nx
        back.append(
            remote(
                comb.at[:, cols_of(e)],
                ret.at[slots(x), :],
                b_send.at[d],
                b_recv.at[d],
                {"ctx": ctx, "exp": e},
            )
        )
    for cp in back:
        cp.start()
    ret[slots(x), :] = comb[:, cols_of(x)]
    for k in range(4):
        for d in (0, 1):
            sum_copy(d, k, 1).wait_send()
    for cp in back:
        cp.wait()
    out_ref[...] = jnp.dot(coll_ref[...], ret[...], preferred_element_type=F32).astype(BF16)


def on_device(
    nz,
    nx,
    queries,
    new_keys,
    new_values,
    cache_keys,
    cache_values,
    offset,
    token_ids,
    expert_table,
    norm_gain,
    w_gate,
    w_up,
    w_down,
):
    T = queries.shape[0]
    cap = T // 2
    width = norm_gain.shape[0]
    QW = queries.shape[1] // 2
    span = cache_keys.shape[0] + new_keys.shape[0]
    ff = w_gate.shape[2]
    chosen = expert_table.at[token_ids].get(mode="promise_in_bounds")
    index = jnp.arange(T, dtype=jnp.int32)
    same = (chosen[:, None] == chosen[None, :]) & (index[None, :] < index[:, None])
    slot = jnp.sum(same.astype(jnp.int32), axis=1)
    target = chosen * cap + slot
    places = jnp.arange(nx * cap, dtype=jnp.int32)
    dispatch = (places[:, None] == target[None, :]).astype(BF16)
    dispatch = jnp.pad(dispatch, ((0, 0), (0, HEAD - T))) if T < HEAD else dispatch
    collect = (target[:, None] == places[None, :]).astype(BF16)
    half = nz // 2
    lanes = 2 * T * (QW // HEAD)
    hbm = pl.BlockSpec(memory_space=pltpu.HBM)
    vmem = pl.BlockSpec(memory_space=pltpu.VMEM)
    dma = pltpu.SemaphoreType.DMA
    return pl.pallas_call(
        functools.partial(layer_kernel, nz, nx),
        out_shape=jax.ShapeDtypeStruct(queries.shape, BF16),
        in_specs=[pl.BlockSpec(memory_space=pltpu.SMEM)] + [hbm] * 6 + [vmem] * 2 + [hbm] * 3,
        out_specs=vmem,
        scratch_shapes=[
            pltpu.VMEM((nz, 2, span, HEAD), BF16),
            pltpu.VMEM((nz, 2, span, HEAD), BF16),
            pltpu.VMEM((2, T, QW), BF16),
            pltpu.VMEM((lanes, HEAD), BF16),
            pltpu.VMEM((2,) + dispatch.shape, BF16),
            pltpu.VMEM((1, lanes), jnp.int32),
            pltpu.VMEM((1, lanes), F32),
            pltpu.VMEM((1, lanes), F32),
            pltpu.VMEM((HEAD, lanes), F32),
            pltpu.VMEM((2 * T, QW), BF16),
            pltpu.VMEM((2, nx * cap, QW), BF16),
            pltpu.VMEM((cap, width), BF16),
            pltpu.VMEM((nz * cap, width), BF16),
            pltpu.VMEM((nz * cap, width), BF16),
            pltpu.VMEM((2, half * cap, width), BF16),
            pltpu.VMEM((4 * cap, ff), F32),
            pltpu.VMEM((2, 4 * cap, ff), BF16),
            pltpu.VMEM((cap, width), BF16),
            pltpu.VMEM((nx * cap, width // nx), BF16),
            pltpu.VMEM((2,) + w_gate.shape[1:], BF16),
            pltpu.VMEM((2,) + w_up.shape[1:], BF16),
            pltpu.VMEM((2,) + w_down.shape[1:], BF16),
            dma((6,)),
            dma((6,)),
            dma((6,)),
            dma((3,)),
            dma((3,)),
            dma((3,)),
            dma((2, 4)),
            dma((2, half, 4)),
            dma((nx, 2)),
            dma((nx, 2)),
            dma((2, 4)),
            dma((2, half, 4)),
            dma((2, 4)),
            dma((2, half, 4)),
            dma((nx,)),
            dma((nx,)),
        ],
        compiler_params=pltpu.CompilerParams(
            collective_id=0, has_side_effects=True, vmem_limit_bytes=VMEM_LIMIT
        ),
    )(
        offset,
        queries,
        new_keys,
        new_values,
        cache_keys,
        cache_values,
        dispatch,
        collect,
        norm_gain.reshape(1, width),
        w_gate,
        w_up,
        w_down,
    )


def solution(mesh):
    split = ("group", "ctx")
    tokens = P(split, "exp")
    placed = (
        tokens,
        tokens,
        tokens,
        tokens,
        tokens,
        P("group"),
        P(split),
        P("group"),
        P(),
        P("exp", None, "ctx"),
        P("exp", None, "ctx"),
        P("exp", "ctx", None),
    )
    return jax.shard_map(
        functools.partial(on_device, mesh.shape["ctx"] // 2, mesh.shape["exp"]),
        mesh=mesh,
        in_specs=placed,
        out_specs=tokens,
        check_vma=False,
    )
```

```python
import functools
import math

import jax
import jax.numpy as jnp
from jax import lax
from jax.experimental import pallas as pl
from jax.experimental.pallas import tpu as pltpu
from jax.sharding import PartitionSpec as P

MESH = pl.DeviceIdType.MESH
F32 = jnp.float32
BF16 = jnp.bfloat16
HEAD = 128
NEG = -1e30
VMEM_LIMIT = 64000 * 1024
LAG = 2


def layer_kernel(
    nz,
    nx,
    offset_ref,
    ids_ref,
    q_hbm,
    nk_hbm,
    nv_hbm,
    ck_hbm,
    cv_hbm,
    table_hbm,
    gain_ref,
    wg_hbm,
    wu_hbm,
    wd_hbm,
    out_ref,
    coll_ref,
    kbuf,
    vbuf,
    qbuf,
    qcat,
    cbuf,
    table,
    found,
    tok_ref,
    m_ref,
    l_ref,
    o_ref,
    att,
    packed,
    arr,
    rows,
    sums,
    rsb,
    gate_s,
    hid,
    comb,
    ret,
    wg,
    wu,
    wd,
    loc_sem,
    pair_send,
    pair_recv,
    w_loc,
    w_send,
    w_recv,
    kv_send,
    kv_recv,
    a_send,
    a_recv,
    g_send,
    g_recv,
    r_send,
    r_recv,
    b_send,
    b_recv,
):
    ctx = lax.axis_index("ctx")
    x = lax.axis_index("exp")
    z = ctx // 2
    c = ctx % 2
    oc = 1 - c
    half = nz // 2
    right = {"ctx": ((z + 1) % nz) * 2 + c, "exp": x}
    left = {"ctx": ((z + nz - 1) % nz) * 2 + c, "exp": x}
    ahead = (right, left)
    pair = {"ctx": z * 2 + oc, "exp": x}
    T = q_hbm.shape[0]
    CK = ck_hbm.shape[0]
    NK = nk_hbm.shape[0]
    QW = qbuf.shape[2]
    group = QW // HEAD
    cap = arr.shape[0]
    width = arr.shape[1]
    hrow = cap // 2
    hcol = width // 2

    def remote(src, dst, ssem, rsem, dev):
        return pltpu.make_async_remote_copy(
            src_ref=src, dst_ref=dst, send_sem=ssem, recv_sem=rsem, device_id=dev, device_id_type=MESH
        )

    kcol = pl.ds(pl.multiple_of(c * HEAD, HEAD), HEAD)
    kcol_o = pl.ds(pl.multiple_of(oc * HEAD, HEAD), HEAD)
    qcol = pl.ds(pl.multiple_of(c * QW, HEAD), QW)
    qcol_o = pl.ds(pl.multiple_of(oc * QW, HEAD), QW)
    parts = (
        (ck_hbm, kbuf, 0, CK),
        (nk_hbm, kbuf, CK, NK),
        (cv_hbm, vbuf, 0, CK),
        (nv_hbm, vbuf, CK, NK),
    )
    local = []
    for i, (src, buf, lo, n) in enumerate(parts):
        local.append(
            pltpu.make_async_copy(src.at[:, kcol], buf.at[0, 0, pl.ds(lo, n), :], loc_sem.at[i])
        )
    local.append(pltpu.make_async_copy(q_hbm.at[:, qcol], qbuf.at[0], loc_sem.at[4]))
    local.append(pltpu.make_async_copy(table_hbm, table, loc_sem.at[5]))
    for cp in local:
        cp.start()

    barrier = pltpu.get_barrier_semaphore()
    others = []
    for d in range(nx):
        for k in range(2):
            if d or k:
                others.append((d, k))
    for dev in ahead:
        pl.semaphore_signal(barrier, inc=1, device_id=dev, device_id_type=MESH)
    for d, k in others:
        pl.semaphore_signal(
            barrier,
            inc=1,
            device_id={"ctx": z * 2 + (c + k) % 2, "exp": (x + d) % nx},
            device_id_type=MESH,
        )
    pl.semaphore_wait(barrier, 2 + len(others))

    swap = []
    for i, (src, buf, lo, n) in enumerate(parts):
        swap.append(
            remote(src.at[:, kcol_o], buf.at[0, 1, pl.ds(lo, n), :], pair_send.at[i], pair_recv.at[i], pair)
        )
    swap.append(remote(q_hbm.at[:, qcol_o], qbuf.at[1], pair_send.at[4], pair_recv.at[4], pair))
    for cp in swap:
        cp.start()

    def last_pos(d, s):
        return 2 * s - 1 if d == 0 else 2 * s - s // half

    def kv_chunk(k, pos):
        return (kbuf, vbuf)[k % 2].at[pos, k // 2]

    def kv_copy(d, k, s, pos):
        return remote(
            kv_chunk(k, pos),
            kv_chunk(k, last_pos(d, s)),
            kv_send.at[d, k],
            kv_recv.at[d, s - 1, k],
            ahead[d],
        )

    for i in range(4):
        local[i].wait()
    for k in (0, 1):
        for d in (0, 1):
            kv_copy(d, k, 1, 0).start()
    local[4].wait()
    for i in range(4):
        swap[i].wait_recv()
    for k in (2, 3):
        for d in (0, 1):
            kv_copy(d, k, 1, 0).start()

    weights = ((wg_hbm, wg), (wu_hbm, wu), (wd_hbm, wd))
    w_own = [pltpu.make_async_copy(src.at[0], dst.at[0], w_loc.at[i]) for i, (src, dst) in enumerate(weights)]
    w_swap = [remote(src.at[0], dst.at[1], w_send.at[i], w_recv.at[i], pair) for i, (src, dst) in enumerate(weights)]
    for cp in w_own:
        cp.start()
    for cp in w_swap:
        cp.start()

    swap[4].wait_recv()
    for g in range(group):
        for s in range(2):
            qcat[pl.ds((g * 2 + s) * T, T), :] = qbuf[s, :, pl.ds(g * HEAD, HEAD)]
    lanes = 2 * T * group
    lane = lax.broadcasted_iota(jnp.int32, (1, lanes), 1)
    bits = T.bit_length() - 1
    second = lax.shift_right_logical(lane, bits) & 1
    tok_ref[...] = z * (2 * T) + (lane & (T - 1)) + jnp.where(second == 0, c, oc) * T
    m_ref[...] = jnp.full_like(m_ref, NEG)
    l_ref[...] = jnp.zeros_like(l_ref)
    o_ref[...] = jnp.zeros_like(o_ref)
    scale = 1.0 / math.sqrt(HEAD)

    local[5].wait()
    one_row = lax.broadcasted_iota(jnp.int32, (1, HEAD), 1)

    def look_up(t, carry):
        name = ids_ref[t]
        line = table[pl.ds(lax.shift_right_logical(name, 7), 1), :]
        found[pl.ds(t, 1), :] = jnp.where(one_row == (name & 127), line, 0)
        return carry

    lax.fori_loop(0, T, look_up, 0)
    chosen = jnp.sum(found[...], axis=1, keepdims=True)
    places = lax.broadcasted_iota(jnp.int32, (T, cbuf.shape[2]), 1)
    onehot = (places == chosen).astype(F32)
    before = (
        lax.broadcasted_iota(jnp.int32, (T, T), 1) < lax.broadcasted_iota(jnp.int32, (T, T), 0)
    ).astype(F32)
    earlier = jnp.dot(before.astype(BF16), onehot.astype(BF16), preferred_element_type=F32)
    slot = jnp.sum(earlier * onehot, axis=1, keepdims=True)
    target = chosen * cap + slot.astype(jnp.int32)
    collect = (places == target).astype(F32).astype(BF16)
    cbuf[0] = collect
    coll_ref[...] = collect
    c_swap = remote(cbuf.at[0], cbuf.at[1], pair_send.at[5], pair_recv.at[5], pair)
    c_swap.start()
    nt = (((1,), (1,)), ((), ()))
    tn = (((0,), (0,)), ((), ()))

    def attend(pos, src, zz):
        owner = zz * 2 + (c if src == 0 else oc)
        s = lax.dot_general(kbuf[pos, src], qcat[...], nt, preferred_element_type=F32) * scale
        crow = lax.broadcasted_iota(jnp.int32, (CK, 1), 0) + owner * CK
        sc = jnp.where(crow < offset_ref[0], s[:CK], NEG)
        nrow = lax.broadcasted_iota(jnp.int32, (NK, lanes), 0) + owner * NK
        sn = jnp.where(nrow <= tok_ref[...], s[CK:], NEG)
        m_old = m_ref[...]
        m_new = jnp.maximum(
            m_old,
            jnp.maximum(jnp.max(sc, axis=0, keepdims=True), jnp.max(sn, axis=0, keepdims=True)),
        )
        pc = jnp.exp(sc - m_new)
        pn = jnp.exp(sn - m_new)
        fade = jnp.exp(m_old - m_new)
        m_ref[...] = m_new
        l_ref[...] = (
            l_ref[...] * fade + jnp.sum(pc, axis=0, keepdims=True) + jnp.sum(pn, axis=0, keepdims=True)
        )
        p = jnp.concatenate([pc.astype(BF16), pn.astype(BF16)], axis=0)
        o_ref[...] = o_ref[...] * fade + lax.dot_general(vbuf[pos, src], p, tn, preferred_element_type=F32)

    def kv_step(s, carry):
        for k in range(4):
            for d in (0, 1):
                here = last_pos(d, s)
                kv_copy(d, k, s, here).wait_recv()
                onward = kv_copy(d, k, s + 1, here)
                if k // 2 == d:
                    onward.wait_send()
                    onward.start()
                else:

                    @pl.when(s < half - 1)
                    def _():
                        onward.wait_send()
                        onward.start()

            if k < 2:

                @pl.when(s > 1)
                def _():
                    attend(2 * s - 3, k, (z + nz - s + 1) % nz)

            else:
                attend(2 * s - 2, k - 2, (z + s - 1) % nz)
        return carry

    lax.fori_loop(1, half, kv_step, 0)
    for k in range(2):
        attend(2 * half - 3, k, (z + nz - half + 1) % nz)
    for k in range(2):
        attend(2 * half - 2, k, (z + half - 1) % nz)
    for d in (0, 1):
        for k in (2 * d, 2 * d + 1):
            kv_copy(d, k, half, 2 * half - 1).wait_recv()
        attend(2 * half - 1, d, (z + half) % nz)
    for k in range(4):
        for d in (0, 1):
            kv_copy(d, k, half, 0).wait_send()
    for cp in swap:
        cp.wait_send()

    done = o_ref[...] / l_ref[...]
    for g in range(group):
        att[:, pl.ds(g * HEAD, HEAD)] = done[:, g * 2 * T : (g + 1) * 2 * T].T.astype(BF16)
    c_swap.wait()
    for k in range(2):
        packed[k] = lax.dot_general(
            cbuf[k], att[pl.ds(k * T, T), :], tn, preferred_element_type=F32
        ).astype(BF16)

    mine = pl.ds(pl.multiple_of((x * 2 + c) * QW, HEAD), QW)

    def slots(e, h):
        return pl.ds(pl.multiple_of(e * cap + h * hrow, hrow), hrow)

    def row_half(h):
        return pl.ds(h * hrow, hrow)

    there = ([], [])
    for h in range(2):
        for d, k in others:
            e = (x + d) % nx
            there[h].append(
                remote(
                    packed.at[k, slots(e, h), :],
                    arr.at[row_half(h), mine],
                    a_send.at[h, d, k],
                    a_recv.at[h, d, k],
                    {"ctx": z * 2 + (c + k) % 2, "exp": e},
                )
            )
        for cp in there[h]:
            cp.start()
        arr[row_half(h), mine] = packed[0, slots(x, h), :]

    lot = nz * hrow

    def part(ref, h, pos, q):
        return ref.at[pl.ds(pl.multiple_of(h * lot + pos * hrow, hrow), hrow), pl.ds(q * hcol, hcol)]

    def normalize(h):
        for cp in there[h]:
            cp.wait_recv()
        v32 = arr[row_half(h), :].astype(F32)
        norm = lax.rsqrt(jnp.mean(v32 * v32, axis=-1, keepdims=True) + 1e-05)
        rows[pl.ds(h * lot, hrow), :] = (v32 * norm * gain_ref[...]).astype(BF16)

    def row_copy(h, q, d, s, pos):
        return remote(
            part(rows, h, pos, q),
            part(rows, h, last_pos(d, s), q),
            g_send.at[d, h * 2 + q],
            g_recv.at[d, s - 1, h * 2 + q],
            ahead[d],
        )

    normalize(0)
    for q in range(2):
        for d in (0, 1):
            row_copy(0, q, d, 1, 0).start()
    normalize(1)
    for cp in w_own:
        cp.wait()
    for cp in w_swap:
        cp.wait()

    M = lot // 2
    ncol = width // 4

    def dense(w, i):
        lo = pl.multiple_of((w % 2) * lot + (w // 2) * M, M)
        if i < 4:
            src = i // 2
            mat = (wg, wu)[i % 2]
            v = lax.dot_general(mat[src], rows[pl.ds(lo, M), :], nt, preferred_element_type=F32)
            if i % 2 == 0:
                gate_s[...] = v
            else:
                g32 = gate_s[...]
                hid[src] = (g32 / (1.0 + jnp.exp(-g32)) * v).T.astype(BF16)
        else:
            cols = pl.ds((i - 4) * ncol, ncol)
            sums[pl.ds(lo, M), cols] = (
                jnp.dot(hid[0], wd[0, :, cols], preferred_element_type=F32)
                + jnp.dot(hid[1], wd[1, :, cols], preferred_element_type=F32)
            ).astype(BF16)

    first_turn = half // 4
    last_turn = (half + LAG) // 2

    def row_pair(j, carry):
        for o in range(2):
            t = 2 * j + 1 + o
            for h in range(2):
                s = t - LAG * h
                for q in range(2):
                    for d in (0, 1):

                        def take(keep=q == d, h=h, q=q, d=d, s=s):
                            here = last_pos(d, s)
                            arrive = row_copy(h, q, d, s, here)
                            onward = row_copy(h, q, d, s + 1, here)

                            def on():
                                onward.wait_send()
                                onward.start()

                            if keep:
                                arrive.wait_recv()
                                pl.when(s < half)(on)
                            else:

                                @pl.when(s < half)
                                def _():
                                    arrive.wait_recv()
                                    pl.when(s < half - 1)(on)

                        if h == 0:
                            pl.when(s <= half)(take)
                        else:
                            pl.when(s > 0)(take)

                            @pl.when(s == 0)
                            def _():
                                row_copy(h, q, d, 1, 0).start()

                    @pl.when(j >= first_turn)
                    def _():
                        dense(j - first_turn, o * 4 + h * 2 + q)

        return carry

    lax.fori_loop(0, last_turn, row_pair, 0)
    for w in range(last_turn - first_turn, 3):
        for i in range(8):
            dense(w, i)
    for cp in there[0] + there[1]:
        cp.wait_send()
    for h in range(2):
        for q in range(2):
            for d in (0, 1):
                row_copy(h, q, d, half, 0).wait_send()

    def sum_copy(h, q, d, s):
        pos = 2 * s - s // half if d == 0 else 2 * s - 1
        return remote(
            part(sums, h, pos, q),
            rsb.at[d, s - 1, row_half(h), pl.ds(q * hcol, hcol)],
            r_send.at[d, h * 2 + q],
            r_recv.at[d, s - 1, h * 2 + q],
            ahead[d],
        )

    def sum_first(h, q, d, s):
        sum_copy(h, q, d, s).start()

    def sum_next(h, q, d, s):
        pos = 2 * s if d == 0 else 2 * s - 1
        sum_copy(h, q, d, s + 1).wait_recv()
        own = part(sums, h, pos, q)
        came = rsb[d, s, row_half(h), pl.ds(q * hcol, hcol)]
        own[...] = (own[...].astype(F32) + came.astype(F32)).astype(BF16)
        sum_copy(h, q, d, s).wait_send()
        sum_copy(h, q, d, s).start()

    def sum_start(h):
        for d in (0, 1):
            sum_first(h, d, d, half)
        for d in (0, 1):
            sum_first(h, 1 - d, d, half - 1)

    def sum_keep(h):
        for d in (0, 1):
            sum_next(h, d, d, half - 1)

    def sum_step(h, s):
        for r in (1, 0):
            for d in (0, 1):
                sum_next(h, d if r == 0 else 1 - d, d, s)

    tw = width // nx

    def cols_of(e):
        return pl.ds(pl.multiple_of(e * tw, HEAD), tw)

    def finish(h):
        for q in range(2):
            for d in (0, 1):
                sum_copy(h, q, d, 1).wait_recv()
            cols = pl.ds(q * hcol, hcol)
            total = part(rows, h, 0, q)[...].astype(F32) + (
                part(sums, h, 0, q)[...].astype(F32)
                + rsb[0, 0, row_half(h), cols].astype(F32)
                + rsb[1, 0, row_half(h), cols].astype(F32)
            )
            comb[row_half(h), cols] = total.astype(BF16)
        back = []
        for d in range(1, nx):
            e = (x + d) % nx
            back.append(
                remote(
                    comb.at[row_half(h), cols_of(e)],
                    ret.at[slots(x, h), :],
                    b_send.at[h, d],
                    b_recv.at[h, d],
                    {"ctx": ctx, "exp": e},
                )
            )
        for cp in back:
            cp.start()
        ret[slots(x, h), :] = comb[row_half(h), cols_of(x)]
        return back

    sum_start(0)
    for i in range(4):
        dense(3, i)
    sum_keep(0)
    for i in range(4, 8):
        dense(3, i)
    sum_step(0, half - 2)
    sum_start(1)
    sum_step(0, half - 3)
    sum_keep(1)

    def sum_both(t, carry):
        sum_step(0, half - 4 - t)
        sum_step(1, half - 2 - t)
        return carry

    lax.fori_loop(0, half - 4, sum_both, 0)
    back = finish(0)
    sum_step(1, 2)
    sum_step(1, 1)
    back = back + finish(1)
    for h in range(2):
        for q in range(2):
            for d in (0, 1):
                sum_copy(h, q, d, 1).wait_send()
    for cp in back:
        cp.wait()
    out_ref[...] = ret[...]


def on_device(
    nz,
    nx,
    queries,
    new_keys,
    new_values,
    cache_keys,
    cache_values,
    offset,
    token_ids,
    expert_table,
    norm_gain,
    w_gate,
    w_up,
    w_down,
):
    T = queries.shape[0]
    cap = T // 2
    width = norm_gain.shape[0]
    QW = queries.shape[1] // 2
    span = cache_keys.shape[0] + new_keys.shape[0]
    ff = w_gate.shape[2]
    half = nz // 2
    lanes = 2 * T * (QW // HEAD)
    hbm = pl.BlockSpec(memory_space=pltpu.HBM)
    vmem = pl.BlockSpec(memory_space=pltpu.VMEM)
    smem = pl.BlockSpec(memory_space=pltpu.SMEM)
    dma = pltpu.SemaphoreType.DMA
    returned, collect = pl.pallas_call(
        functools.partial(layer_kernel, nz, nx),
        out_shape=(
            jax.ShapeDtypeStruct((nx * cap, width // nx), BF16),
            jax.ShapeDtypeStruct((T, nx * cap), BF16),
        ),
        in_specs=[smem] * 2 + [hbm] * 6 + [vmem] + [hbm] * 3,
        out_specs=(vmem, vmem),
        scratch_shapes=[
            pltpu.VMEM((nz, 2, span, HEAD), BF16),
            pltpu.VMEM((nz, 2, span, HEAD), BF16),
            pltpu.VMEM((2, T, QW), BF16),
            pltpu.VMEM((lanes, HEAD), BF16),
            pltpu.VMEM((2, T, nx * cap), BF16),
            pltpu.VMEM((expert_table.shape[0] // HEAD, HEAD), jnp.int32),
            pltpu.VMEM((T, HEAD), jnp.int32),
            pltpu.VMEM((1, lanes), jnp.int32),
            pltpu.VMEM((1, lanes), F32),
            pltpu.VMEM((1, lanes), F32),
            pltpu.VMEM((HEAD, lanes), F32),
            pltpu.VMEM((2 * T, QW), BF16),
            pltpu.VMEM((2, nx * cap, QW), BF16),
            pltpu.VMEM((cap, width), BF16),
            pltpu.VMEM((nz * cap, width), BF16),
            pltpu.VMEM((nz * cap, width), BF16),
            pltpu.VMEM((2, half, cap, width), BF16),
            pltpu.VMEM((ff, nz * cap // 4), F32),
            pltpu.VMEM((2, nz * cap // 4, ff), BF16),
            pltpu.VMEM((cap, width), BF16),
            pltpu.VMEM((nx * cap, width // nx), BF16),
            pltpu.VMEM((2, ff, width), BF16),
            pltpu.VMEM((2, ff, width), BF16),
            pltpu.VMEM((2,) + w_down.shape[1:], BF16),
            dma((6,)),
            dma((6,)),
            dma((6,)),
            dma((3,)),
            dma((3,)),
            dma((3,)),
            dma((2, 4)),
            dma((2, half, 4)),
            dma((2, nx, 2)),
            dma((2, nx, 2)),
            dma((2, 4)),
            dma((2, half, 4)),
            dma((2, 4)),
            dma((2, half, 4)),
            dma((2, nx)),
            dma((2, nx)),
        ],
        compiler_params=pltpu.CompilerParams(
            collective_id=0, has_side_effects=True, vmem_limit_bytes=VMEM_LIMIT
        ),
    )(
        offset,
        token_ids,
        queries,
        new_keys,
        new_values,
        cache_keys,
        cache_values,
        expert_table.reshape(-1, HEAD),
        norm_gain.reshape(1, width),
        jnp.swapaxes(w_gate, 1, 2),
        jnp.swapaxes(w_up, 1, 2),
        w_down,
    )
    return jnp.dot(collect, returned, preferred_element_type=F32).astype(BF16)


def solution(mesh):
    split = ("group", "ctx")
    tokens = P(split, "exp")
    placed = (
        tokens,
        tokens,
        tokens,
        tokens,
        tokens,
        P("group"),
        P(split),
        P("group"),
        P(),
        P("exp", None, "ctx"),
        P("exp", None, "ctx"),
        P("exp", "ctx", None),
    )
    return jax.shard_map(
        functools.partial(on_device, mesh.shape["ctx"] // 2, mesh.shape["exp"]),
        mesh=mesh,
        in_specs=placed,
        out_specs=tokens,
        check_vma=False,
    )
```

```python
import functools
import math

import jax
import jax.numpy as jnp
from jax import lax
from jax.experimental import pallas as pl
from jax.experimental.pallas import tpu as pltpu
from jax.sharding import PartitionSpec as P

MESH = pl.DeviceIdType.MESH
F32 = jnp.float32
BF16 = jnp.bfloat16
HEAD = 128
NEG = -1e30
VMEM_LIMIT = 64000 * 1024


def layer_kernel(
    nz,
    nx,
    offset_ref,
    ids_ref,
    q_hbm,
    nk_hbm,
    nv_hbm,
    ck_hbm,
    cv_hbm,
    table_hbm,
    gain_ref,
    wg_hbm,
    wu_hbm,
    wd_hbm,
    out_ref,
    kbuf,
    vbuf,
    qbuf,
    qcat,
    cbuf,
    table,
    found,
    tok_ref,
    m_ref,
    l_ref,
    o_ref,
    att,
    packed,
    arr,
    rows,
    sums,
    rsb,
    acc,
    hid,
    comb,
    ret,
    wg,
    wu,
    wd,
    loc_sem,
    pair_send,
    pair_recv,
    w_loc,
    w_send,
    w_recv,
    kv_send,
    kv_recv,
    a_send,
    a_recv,
    g_send,
    g_recv,
    r_send,
    r_recv,
    b_send,
    b_recv,
):
    ctx = lax.axis_index("ctx")
    x = lax.axis_index("exp")
    z = ctx // 2
    c = ctx % 2
    oc = 1 - c
    half = nz // 2
    right = {"ctx": ((z + 1) % nz) * 2 + c, "exp": x}
    left = {"ctx": ((z + nz - 1) % nz) * 2 + c, "exp": x}
    ahead = (right, left)
    pair = {"ctx": z * 2 + oc, "exp": x}
    T = q_hbm.shape[0]
    CK = ck_hbm.shape[0]
    NK = nk_hbm.shape[0]
    QW = qbuf.shape[2]
    group = QW // HEAD
    cap = arr.shape[0]
    width = arr.shape[1]
    hrow = cap // 2
    hcol = width // 2

    def remote(src, dst, ssem, rsem, dev):
        return pltpu.make_async_remote_copy(
            src_ref=src, dst_ref=dst, send_sem=ssem, recv_sem=rsem, device_id=dev, device_id_type=MESH
        )

    kcol = pl.ds(pl.multiple_of(c * HEAD, HEAD), HEAD)
    kcol_o = pl.ds(pl.multiple_of(oc * HEAD, HEAD), HEAD)
    qcol = pl.ds(pl.multiple_of(c * QW, HEAD), QW)
    qcol_o = pl.ds(pl.multiple_of(oc * QW, HEAD), QW)
    parts = (
        (ck_hbm, kbuf, 0, CK),
        (nk_hbm, kbuf, CK, NK),
        (cv_hbm, vbuf, 0, CK),
        (nv_hbm, vbuf, CK, NK),
    )
    local = []
    for i, (src, buf, lo, n) in enumerate(parts):
        local.append(
            pltpu.make_async_copy(src.at[:, kcol], buf.at[0, 0, pl.ds(lo, n), :], loc_sem.at[i])
        )
    local.append(pltpu.make_async_copy(q_hbm.at[:, qcol], qbuf.at[0], loc_sem.at[4]))
    local.append(pltpu.make_async_copy(table_hbm, table, loc_sem.at[5]))
    for cp in local:
        cp.start()

    barrier = pltpu.get_barrier_semaphore()
    others = []
    for d in range(nx):
        for k in range(2):
            if d or k:
                others.append((d, k))
    for dev in ahead:
        pl.semaphore_signal(barrier, inc=1, device_id=dev, device_id_type=MESH)
    for d, k in others:
        pl.semaphore_signal(
            barrier,
            inc=1,
            device_id={"ctx": z * 2 + (c + k) % 2, "exp": (x + d) % nx},
            device_id_type=MESH,
        )
    pl.semaphore_wait(barrier, 2 + len(others))

    swap = []
    for i, (src, buf, lo, n) in enumerate(parts):
        swap.append(
            remote(src.at[:, kcol_o], buf.at[0, 1, pl.ds(lo, n), :], pair_send.at[i], pair_recv.at[i], pair)
        )
    swap.append(remote(q_hbm.at[:, qcol_o], qbuf.at[1], pair_send.at[4], pair_recv.at[4], pair))
    for cp in swap:
        cp.start()

    def last_pos(d, s):
        return 2 * s - 1 if d == 0 else 2 * s - s // half

    def kv_chunk(k, pos):
        return (kbuf, vbuf)[k % 2].at[pos, k // 2]

    def kv_copy(d, k, s, pos):
        return remote(
            kv_chunk(k, pos),
            kv_chunk(k, last_pos(d, s)),
            kv_send.at[d, k],
            kv_recv.at[d, s - 1, k],
            ahead[d],
        )

    for i in range(4):
        local[i].wait()
    for k in (0, 1):
        for d in (0, 1):
            kv_copy(d, k, 1, 0).start()
    local[4].wait()
    for i in range(4):
        swap[i].wait_recv()
    for k in (2, 3):
        for d in (0, 1):
            kv_copy(d, k, 1, 0).start()

    weights = ((wg_hbm, wg), (wu_hbm, wu), (wd_hbm, wd))
    w_own = [pltpu.make_async_copy(src.at[0], dst.at[0], w_loc.at[i]) for i, (src, dst) in enumerate(weights)]
    w_swap = [remote(src.at[0], dst.at[1], w_send.at[i], w_recv.at[i], pair) for i, (src, dst) in enumerate(weights)]
    for cp in w_own:
        cp.start()
    for cp in w_swap:
        cp.start()

    swap[4].wait_recv()
    for g in range(group):
        for s in range(2):
            qcat[pl.ds((g * 2 + s) * T, T), :] = qbuf[s, :, pl.ds(g * HEAD, HEAD)]
    lanes = 2 * T * group
    lane = lax.broadcasted_iota(jnp.int32, (1, lanes), 1)
    bits = T.bit_length() - 1
    second = lax.shift_right_logical(lane, bits) & 1
    tok_ref[...] = z * (2 * T) + (lane & (T - 1)) + jnp.where(second == 0, c, oc) * T
    m_ref[...] = jnp.full_like(m_ref, NEG)
    l_ref[...] = jnp.zeros_like(l_ref)
    o_ref[...] = jnp.zeros_like(o_ref)
    scale = 1.0 / math.sqrt(HEAD)
    local[5].wait()
    one_row = lax.broadcasted_iota(jnp.int32, (1, HEAD), 1)

    def look_up(t, carry):
        name = ids_ref[t]
        line = table[pl.ds(lax.shift_right_logical(name, 7), 1), :]
        found[pl.ds(t, 1), :] = jnp.where(one_row == (name & 127), line, 0)
        return carry

    lax.fori_loop(0, T, look_up, 0)
    chosen = jnp.sum(found[...], axis=1, keepdims=True)
    places = lax.broadcasted_iota(jnp.int32, (T, cbuf.shape[2]), 1)
    onehot = (places == chosen).astype(F32)
    before = (
        lax.broadcasted_iota(jnp.int32, (T, T), 1) < lax.broadcasted_iota(jnp.int32, (T, T), 0)
    ).astype(F32)
    earlier = jnp.dot(before.astype(BF16), onehot.astype(BF16), preferred_element_type=F32)
    slot = jnp.sum(earlier * onehot, axis=1, keepdims=True)
    target = chosen * cap + slot.astype(jnp.int32)
    collect = (places == target).astype(F32).astype(BF16)
    cbuf[0] = collect
    c_swap = remote(cbuf.at[0], cbuf.at[1], pair_send.at[5], pair_recv.at[5], pair)
    c_swap.start()
    nt = (((1,), (1,)), ((), ()))
    tn = (((0,), (0,)), ((), ()))

    def attend(pos, src, zz):
        owner = zz * 2 + (c if src == 0 else oc)
        s = lax.dot_general(kbuf[pos, src], qcat[...], nt, preferred_element_type=F32) * scale
        crow = lax.broadcasted_iota(jnp.int32, (CK, 1), 0) + owner * CK
        sc = jnp.where(crow < offset_ref[...], s[:CK], NEG)
        nrow = lax.broadcasted_iota(jnp.int32, (NK, lanes), 0) + owner * NK
        sn = jnp.where(nrow <= tok_ref[...], s[CK:], NEG)
        m_old = m_ref[...]
        m_new = jnp.maximum(
            m_old,
            jnp.maximum(jnp.max(sc, axis=0, keepdims=True), jnp.max(sn, axis=0, keepdims=True)),
        )
        pc = jnp.exp(sc - m_new)
        pn = jnp.exp(sn - m_new)
        fade = jnp.exp(m_old - m_new)
        m_ref[...] = m_new
        l_ref[...] = (
            l_ref[...] * fade + jnp.sum(pc, axis=0, keepdims=True) + jnp.sum(pn, axis=0, keepdims=True)
        )
        p = jnp.concatenate([pc.astype(BF16), pn.astype(BF16)], axis=0)
        o_ref[...] = o_ref[...] * fade + lax.dot_general(vbuf[pos, src], p, tn, preferred_element_type=F32)

    def turned(k, d):
        return (k + 2 * d) % 4

    def kv_step(s, carry):
        for i in range(4):
            for d in (0, 1):
                k = turned(i, d)
                here = last_pos(d, s)
                kv_copy(d, k, s, here).wait_recv()
                onward = kv_copy(d, k, s + 1, here)
                if k // 2 == d:
                    onward.wait_send()
                    onward.start()
                else:

                    @pl.when(s < half - 1)
                    def _():
                        onward.wait_send()
                        onward.start()

            if i < 2:

                @pl.when(s > 1)
                def _():
                    attend(2 * s - 3, i, (z + nz - s + 1) % nz)

            else:
                attend(2 * s - 2, i - 2, (z + s - 1) % nz)
        return carry

    lax.fori_loop(1, half, kv_step, 0)
    for k in range(2):
        attend(2 * half - 3, k, (z + nz - half + 1) % nz)
    for k in range(2):
        attend(2 * half - 2, k, (z + half - 1) % nz)
    for d in (0, 1):
        for k in (2 * d, 2 * d + 1):
            kv_copy(d, k, half, 2 * half - 1).wait_recv()
        attend(2 * half - 1, d, (z + half) % nz)
    for k in range(4):
        for d in (0, 1):
            kv_copy(d, k, half, 0).wait_send()
    for cp in swap:
        cp.wait_send()

    done = o_ref[...] / l_ref[...]
    for g in range(group):
        att[:, pl.ds(g * HEAD, HEAD)] = done[:, g * 2 * T : (g + 1) * 2 * T].T.astype(BF16)
    c_swap.wait()
    for k in range(2):
        packed[k] = lax.dot_general(
            cbuf[k], att[pl.ds(k * T, T), :], tn, preferred_element_type=F32
        ).astype(BF16)

    mine = pl.ds(pl.multiple_of((x * 2 + c) * QW, HEAD), QW)

    def slots(e, h):
        return pl.ds(pl.multiple_of(e * cap + h * hrow, hrow), hrow)

    def row_half(h):
        return pl.ds(h * hrow, hrow)

    there = ([], [])
    for h in range(2):
        for d, k in others:
            e = (x + d) % nx
            there[h].append(
                remote(
                    packed.at[k, slots(e, h), :],
                    arr.at[row_half(h), mine],
                    a_send.at[h, d, k],
                    a_recv.at[h, d, k],
                    {"ctx": z * 2 + (c + k) % 2, "exp": e},
                )
            )
        for cp in there[h]:
            cp.start()
        arr[row_half(h), mine] = packed[0, slots(x, h), :]

    def normalize(h):
        for cp in there[h]:
            cp.wait_recv()
        v32 = arr[row_half(h), :].astype(F32)
        norm = lax.rsqrt(jnp.mean(v32 * v32, axis=-1, keepdims=True) + 1e-05)
        rows[row_half(h), :] = (v32 * norm * gain_ref[...]).astype(BF16)

    def part(ref, pos, k):
        return ref.at[
            pl.ds(pl.multiple_of(pos * cap + (k // 2) * hrow, hrow), hrow), pl.ds((k % 2) * hcol, hcol)
        ]

    def row_copy(d, k, s, pos):
        return remote(
            part(rows, pos, k),
            part(rows, last_pos(d, s), k),
            g_send.at[d, k],
            g_recv.at[d, s - 1, k],
            ahead[d],
        )

    for h in range(2):
        normalize(h)
        for k in (2 * h, 2 * h + 1):
            for d in (0, 1):
                row_copy(d, k, 1, 0).start()
    for cp in w_own:
        cp.wait()
    for cp in w_swap:
        cp.wait()

    M = 4 * cap
    ncols = 4
    ncol = width // ncols

    def activate(src):
        g32 = acc[2 * src]
        hid[src] = (g32 / (1.0 + jnp.exp(-g32)) * acc[2 * src + 1]).T.astype(BF16)

    def project(g, i, cols):
        return lax.dot_general(
            (wg, wu)[i % 2][i // 2, :, cols],
            rows[pl.ds(pl.multiple_of(g * M, M), M), cols],
            nt,
            preferred_element_type=F32,
        )

    def dense(g, i):
        if i < 4:
            acc[i] = project(g, i, pl.ds(0, width))
            if i % 2:
                activate(i // 2)
        else:
            cols = pl.ds((i - 4) * ncol, ncol)
            sums[pl.ds(pl.multiple_of(g * M, M), M), cols] = (
                jnp.dot(hid[0], wd[0, :, cols], preferred_element_type=F32)
                + jnp.dot(hid[1], wd[1, :, cols], preferred_element_type=F32)
            ).astype(BF16)

    pairs = half // 2

    def row_step(s, last):
        for i in range(4):
            for d in (0, 1):
                k = turned(i, d)
                here = last_pos(d, s)
                row_copy(d, k, s, here).wait_recv()
                if not last or k // 2 == d:
                    onward = row_copy(d, k, s + 1, here)
                    onward.wait_send()
                    onward.start()
            yield i

    def row_pair(j, carry):
        for o in range(2):
            for k in row_step(2 * j + 1 + o, False):

                @pl.when(j > 0)
                def _():
                    dense(j - 1, o * 4 + k)

        return carry

    lax.fori_loop(0, pairs - 1, row_pair, 0)
    tail = pairs - 1
    for i in row_step(half - 1, True):
        if i == 1 and tail > 0:
            for piece in range(8):
                dense(tail - 1, piece)
    for q in range(2):
        for d in (0, 1):
            row_copy(d, 2 * d + q, half, 2 * half - 1).wait_recv()
        cols = pl.ds(q * hcol, hcol)
        for i in range(4):
            v = project(tail, i, cols)
            acc[i] = v if q == 0 else acc[i] + v
    for src in range(2):
        activate(src)

    def sum_copy(d, k, s):
        pos = 2 * s - s // half if d == 0 else 2 * s - 1
        return remote(
            part(sums, pos, k),
            part(rsb.at[d], s - 1, k),
            r_send.at[d, k],
            r_recv.at[d, s - 1, k],
            ahead[d],
        )

    for q in range(2):
        for i in (4 + 2 * q, 5 + 2 * q):
            dense(tail, i)
        for d in (0, 1):
            sum_copy(d, 2 * d + q, half).start()

    def add_in(d, k, s):
        pos = 2 * s if d == 0 else 2 * s - 1
        sum_copy(d, k, s + 1).wait_recv()
        own = part(sums, pos, k)
        own[...] = (own[...].astype(F32) + part(rsb.at[d], s, k)[...].astype(F32)).astype(BF16)

    def sum_step(t, carry):
        s = half - 1 - t
        for q in range(2):
            for d in (0, 1):
                k = 2 * (1 - d) + q

                @pl.when(t > 0)
                def _():
                    add_in(d, k, s)
                    sum_copy(d, k, s).wait_send()

                sum_copy(d, k, s).start()
        for q in range(2):
            for d in (0, 1):
                k = 2 * d + q
                add_in(d, k, s)
                sum_copy(d, k, s).wait_send()
                sum_copy(d, k, s).start()
        return carry

    lax.fori_loop(0, half - 1, sum_step, 0)

    tw = width // nx
    each = hcol // tw

    def give_back(e, sends):
        cols = pl.ds(e * tw, tw)
        there_x = pl.ds(pl.multiple_of(x * cap, cap), cap)
        step = (e - x + nx) % nx

        @pl.when(e != x)
        def _():
            move = remote(
                comb.at[:, cols],
                ret.at[there_x, :],
                b_send.at[step],
                b_recv.at[step],
                {"ctx": ctx, "exp": e},
            )
            if sends:
                move.start()
            else:
                move.wait_send()

        if sends:

            @pl.when(e == x)
            def _():
                ret[there_x, :] = comb[:, cols]

    for q in range(2):
        for h in range(2):
            k = 2 * h + q
            for d in (0, 1):
                sum_copy(d, k, 1).wait_recv()
            total = part(rows, 0, k)[...].astype(F32) + (
                part(sums, 0, k)[...].astype(F32)
                + part(rsb.at[0], 0, k)[...].astype(F32)
                + part(rsb.at[1], 0, k)[...].astype(F32)
            )
            part(comb, 0, k)[...] = total.astype(BF16)
        for e in range(q * each, (q + 1) * each):
            give_back(e, True)
    for cp in there[0] + there[1]:
        cp.wait_send()
    for k in range(4):
        for d in (0, 1):
            row_copy(d, k, half, 0).wait_send()
            sum_copy(d, k, 1).wait_send()
    for e in range(nx):
        give_back(e, False)
    for d in range(1, nx):
        e = (x + nx - d) % nx
        spot = pl.ds(pl.multiple_of(e * cap, cap), cap)
        remote(comb.at[:, pl.ds(0, tw)], ret.at[spot, :], b_send.at[d], b_recv.at[d], {"ctx": ctx, "exp": e}).wait_recv()
    out_ref[...] = jnp.dot(cbuf[0], ret[...], preferred_element_type=F32).astype(BF16)


def on_device(
    nz,
    nx,
    queries,
    new_keys,
    new_values,
    cache_keys,
    cache_values,
    offset,
    token_ids,
    expert_table,
    norm_gain,
    w_gate,
    w_up,
    w_down,
):
    T = queries.shape[0]
    cap = T // 2
    width = norm_gain.shape[0]
    QW = queries.shape[1] // 2
    span = cache_keys.shape[0] + new_keys.shape[0]
    ff = w_gate.shape[2]
    half = nz // 2
    lanes = 2 * T * (QW // HEAD)
    hbm = pl.BlockSpec(memory_space=pltpu.HBM)
    vmem = pl.BlockSpec(memory_space=pltpu.VMEM)
    smem = pl.BlockSpec(memory_space=pltpu.SMEM)
    dma = pltpu.SemaphoreType.DMA
    return pl.pallas_call(
        functools.partial(layer_kernel, nz, nx),
        out_shape=jax.ShapeDtypeStruct(queries.shape, BF16),
        in_specs=[vmem, smem] + [hbm] * 6 + [vmem] + [hbm] * 3,
        out_specs=vmem,
        scratch_shapes=[
            pltpu.VMEM((nz, 2, span, HEAD), BF16),
            pltpu.VMEM((nz, 2, span, HEAD), BF16),
            pltpu.VMEM((2, T, QW), BF16),
            pltpu.VMEM((lanes, HEAD), BF16),
            pltpu.VMEM((2, T, nx * cap), BF16),
            pltpu.VMEM((expert_table.shape[0] // HEAD, HEAD), jnp.int32),
            pltpu.VMEM((T, HEAD), jnp.int32),
            pltpu.VMEM((1, lanes), jnp.int32),
            pltpu.VMEM((1, lanes), F32),
            pltpu.VMEM((1, lanes), F32),
            pltpu.VMEM((HEAD, lanes), F32),
            pltpu.VMEM((2 * T, QW), BF16),
            pltpu.VMEM((2, nx * cap, QW), BF16),
            pltpu.VMEM((cap, width), BF16),
            pltpu.VMEM((nz * cap, width), BF16),
            pltpu.VMEM((nz * cap, width), BF16),
            pltpu.VMEM((2, half * cap, width), BF16),
            pltpu.VMEM((4, ff, 4 * cap), F32),
            pltpu.VMEM((2, 4 * cap, ff), BF16),
            pltpu.VMEM((cap, width), BF16),
            pltpu.VMEM((nx * cap, width // nx), BF16),
            pltpu.VMEM((2, ff, width), BF16),
            pltpu.VMEM((2, ff, width), BF16),
            pltpu.VMEM((2,) + w_down.shape[1:], BF16),
            dma((6,)),
            dma((6,)),
            dma((6,)),
            dma((3,)),
            dma((3,)),
            dma((3,)),
            dma((2, 4)),
            dma((2, half, 4)),
            dma((2, nx, 2)),
            dma((2, nx, 2)),
            dma((2, 4)),
            dma((2, half, 4)),
            dma((2, 4)),
            dma((2, half, 4)),
            dma((nx,)),
            dma((nx,)),
        ],
        compiler_params=pltpu.CompilerParams(
            collective_id=0, has_side_effects=True, vmem_limit_bytes=VMEM_LIMIT
        ),
    )(
        offset.reshape(1, 1),
        token_ids,
        queries,
        new_keys,
        new_values,
        cache_keys,
        cache_values,
        expert_table.reshape(-1, HEAD),
        norm_gain.reshape(1, width),
        jnp.swapaxes(w_gate, 1, 2),
        jnp.swapaxes(w_up, 1, 2),
        w_down,
    )


def solution(mesh):
    split = ("group", "ctx")
    tokens = P(split, "exp")
    placed = (
        tokens,
        tokens,
        tokens,
        tokens,
        tokens,
        P("group"),
        P(split),
        P("group"),
        P(),
        P("exp", None, "ctx"),
        P("exp", None, "ctx"),
        P("exp", "ctx", None),
    )
    return jax.shard_map(
        functools.partial(on_device, mesh.shape["ctx"] // 2, mesh.shape["exp"]),
        mesh=mesh,
        in_specs=placed,
        out_specs=tokens,
        check_vma=False,
    )
```

```python
import functools
import math

import jax
import jax.numpy as jnp
from jax import lax
from jax.experimental import pallas as pl
from jax.experimental.pallas import tpu as pltpu
from jax.sharding import PartitionSpec as P

MESH = pl.DeviceIdType.MESH
F32 = jnp.float32
BF16 = jnp.bfloat16
HEAD = 128
NEG = -1e30
VMEM_LIMIT = 64000 * 1024


def layer_kernel(
    nz,
    nx,
    offset_ref,
    ids_ref,
    q_hbm,
    nk_hbm,
    nv_hbm,
    ck_hbm,
    cv_hbm,
    table_hbm,
    gain_hbm,
    wg_hbm,
    wu_hbm,
    wd_hbm,
    out_ref,
    kbuf,
    vbuf,
    qbuf,
    qcat,
    cbuf,
    table,
    found,
    gain_ref,
    tok_ref,
    m_ref,
    l_ref,
    o_ref,
    att,
    packed,
    arr,
    rows,
    sums,
    rsb,
    acc,
    hid,
    comb,
    ret,
    wg,
    wu,
    wd,
    loc_sem,
    pair_send,
    pair_recv,
    w_loc,
    w_send,
    w_recv,
    kv_send,
    kv_recv,
    a_send,
    a_recv,
    g_send,
    g_recv,
    r_send,
    r_recv,
    b_send,
    b_recv,
):
    ctx = lax.axis_index("ctx")
    x = lax.axis_index("exp")
    z = ctx // 2
    c = ctx % 2
    oc = 1 - c
    half = nz // 2
    right = {"ctx": ((z + 1) % nz) * 2 + c, "exp": x}
    left = {"ctx": ((z + nz - 1) % nz) * 2 + c, "exp": x}
    ahead = (right, left)
    pair = {"ctx": z * 2 + oc, "exp": x}
    T = q_hbm.shape[0]
    CK = ck_hbm.shape[0]
    NK = nk_hbm.shape[0]
    QW = qbuf.shape[2]
    group = QW // HEAD
    cap = arr.shape[0]
    width = arr.shape[1]
    hrow = cap // 2
    hcol = width // 2

    def remote(src, dst, ssem, rsem, dev):
        return pltpu.make_async_remote_copy(
            src_ref=src, dst_ref=dst, send_sem=ssem, recv_sem=rsem, device_id=dev, device_id_type=MESH
        )

    kcol = pl.ds(pl.multiple_of(c * HEAD, HEAD), HEAD)
    kcol_o = pl.ds(pl.multiple_of(oc * HEAD, HEAD), HEAD)
    qcol = pl.ds(pl.multiple_of(c * QW, HEAD), QW)
    qcol_o = pl.ds(pl.multiple_of(oc * QW, HEAD), QW)
    parts = (
        (ck_hbm, kbuf, 0, CK),
        (nk_hbm, kbuf, CK, NK),
        (cv_hbm, vbuf, 0, CK),
        (nv_hbm, vbuf, CK, NK),
    )
    local = []
    for i, (src, buf, lo, n) in enumerate(parts):
        local.append(
            pltpu.make_async_copy(src.at[:, kcol], buf.at[0, 0, pl.ds(lo, n), :], loc_sem.at[i])
        )
    local.append(pltpu.make_async_copy(q_hbm.at[:, qcol], qbuf.at[0], loc_sem.at[4]))
    local.append(pltpu.make_async_copy(table_hbm, table, loc_sem.at[5]))
    local.append(pltpu.make_async_copy(gain_hbm, gain_ref, loc_sem.at[6]))
    barrier = pltpu.get_barrier_semaphore()
    others = []
    for d in range(nx):
        for k in range(2):
            if d or k:
                others.append((d, k))
    for dev in ahead:
        pl.semaphore_signal(barrier, inc=1, device_id=dev, device_id_type=MESH)
    for d, k in others:
        pl.semaphore_signal(
            barrier,
            inc=1,
            device_id={"ctx": z * 2 + (c + k) % 2, "exp": (x + d) % nx},
            device_id_type=MESH,
        )
    for cp in local:
        cp.start()
    pl.semaphore_wait(barrier, 2 + len(others))

    swap = []
    for i, (src, buf, lo, n) in enumerate(parts):
        swap.append(
            remote(src.at[:, kcol_o], buf.at[0, 1, pl.ds(lo, n), :], pair_send.at[i], pair_recv.at[i], pair)
        )
    swap.append(remote(q_hbm.at[:, qcol_o], qbuf.at[1], pair_send.at[4], pair_recv.at[4], pair))
    for cp in swap:
        cp.start()

    def last_pos(d, s):
        return 2 * s - 1 if d == 0 else 2 * s - s // half

    def kv_chunk(k, pos):
        return (kbuf, vbuf)[k % 2].at[pos, k // 2]

    def kv_copy(d, k, s, pos):
        return remote(
            kv_chunk(k, pos),
            kv_chunk(k, last_pos(d, s)),
            kv_send.at[d, k],
            kv_recv.at[d, s - 1, k],
            ahead[d],
        )

    for i in range(4):
        local[i].wait()
    for k in (0, 1):
        for d in (0, 1):
            kv_copy(d, k, 1, 0).start()
    local[4].wait()
    for i in range(4):
        swap[i].wait_recv()
    for k in (2, 3):
        for d in (0, 1):
            kv_copy(d, k, 1, 0).start()

    weights = ((wg_hbm, wg), (wu_hbm, wu), (wd_hbm, wd))
    w_own = [pltpu.make_async_copy(src.at[0], dst.at[0], w_loc.at[i]) for i, (src, dst) in enumerate(weights)]
    w_swap = [remote(src.at[0], dst.at[1], w_send.at[i], w_recv.at[i], pair) for i, (src, dst) in enumerate(weights)]
    for cp in w_own:
        cp.start()
    for cp in w_swap:
        cp.start()

    swap[4].wait_recv()
    for g in range(group):
        for s in range(2):
            qcat[pl.ds((g * 2 + s) * T, T), :] = qbuf[s, :, pl.ds(g * HEAD, HEAD)]
    lanes = 2 * T * group
    lane = lax.broadcasted_iota(jnp.int32, (1, lanes), 1)
    bits = T.bit_length() - 1
    second = lax.shift_right_logical(lane, bits) & 1
    tok_ref[...] = z * (2 * T) + (lane & (T - 1)) + jnp.where(second == 0, c, oc) * T
    m_ref[...] = jnp.full_like(m_ref, NEG)
    l_ref[...] = jnp.zeros_like(l_ref)
    o_ref[...] = jnp.zeros_like(o_ref)
    scale = 1.0 / math.sqrt(HEAD)
    local[5].wait()
    local[6].wait()
    one_row = lax.broadcasted_iota(jnp.int32, (1, HEAD), 1)

    def look_up(t, carry):
        name = ids_ref[t]
        line = table[pl.ds(lax.shift_right_logical(name, 7), 1), :]
        found[pl.ds(t, 1), :] = jnp.where(one_row == (name & 127), line, 0)
        return carry

    lax.fori_loop(0, T, look_up, 0)
    chosen = jnp.sum(found[...], axis=1, keepdims=True)
    places = lax.broadcasted_iota(jnp.int32, (T, cbuf.shape[2]), 1)
    onehot = (places == chosen).astype(F32)
    before = (
        lax.broadcasted_iota(jnp.int32, (T, T), 1) < lax.broadcasted_iota(jnp.int32, (T, T), 0)
    ).astype(F32)
    earlier = jnp.dot(before.astype(BF16), onehot.astype(BF16), preferred_element_type=F32)
    slot = jnp.sum(earlier * onehot, axis=1, keepdims=True)
    target = chosen * cap + slot.astype(jnp.int32)
    collect = (places == target).astype(F32).astype(BF16)
    cbuf[0] = collect
    c_swap = remote(cbuf.at[0], cbuf.at[1], pair_send.at[5], pair_recv.at[5], pair)
    c_swap.start()
    nt = (((1,), (1,)), ((), ()))
    tn = (((0,), (0,)), ((), ()))

    def attend(pos, src, zz):
        owner = zz * 2 + (c if src == 0 else oc)
        s = lax.dot_general(kbuf[pos, src], qcat[...], nt, preferred_element_type=F32) * scale
        crow = lax.broadcasted_iota(jnp.int32, (CK, 1), 0) + owner * CK
        sc = jnp.where(crow < offset_ref[...], s[:CK], NEG)
        nrow = lax.broadcasted_iota(jnp.int32, (NK, lanes), 0) + owner * NK
        sn = jnp.where(nrow <= tok_ref[...], s[CK:], NEG)
        m_old = m_ref[...]
        m_new = jnp.maximum(
            m_old,
            jnp.maximum(jnp.max(sc, axis=0, keepdims=True), jnp.max(sn, axis=0, keepdims=True)),
        )
        pc = jnp.exp(sc - m_new)
        pn = jnp.exp(sn - m_new)
        fade = jnp.exp(m_old - m_new)
        m_ref[...] = m_new
        l_ref[...] = (
            l_ref[...] * fade + jnp.sum(pc, axis=0, keepdims=True) + jnp.sum(pn, axis=0, keepdims=True)
        )
        p = jnp.concatenate([pc.astype(BF16), pn.astype(BF16)], axis=0)
        o_ref[...] = o_ref[...] * fade + lax.dot_general(vbuf[pos, src], p, tn, preferred_element_type=F32)

    def turned(k, d):
        return (k + 2 * d) % 4

    def kv_step(s, carry):
        for i in range(4):
            for d in (0, 1):
                k = turned(i, d)
                here = last_pos(d, s)
                kv_copy(d, k, s, here).wait_recv()
                onward = kv_copy(d, k, s + 1, here)
                if k // 2 == d:
                    onward.wait_send()
                    onward.start()
                else:

                    @pl.when(s < half - 1)
                    def _():
                        onward.wait_send()
                        onward.start()

            if i < 2:

                @pl.when(s > 1)
                def _():
                    attend(2 * s - 3, i, (z + nz - s + 1) % nz)

            else:
                attend(2 * s - 2, i - 2, (z + s - 1) % nz)
        return carry

    lax.fori_loop(1, half, kv_step, 0)
    for k in range(2):
        attend(2 * half - 3, k, (z + nz - half + 1) % nz)
    for k in range(2):
        attend(2 * half - 2, k, (z + half - 1) % nz)
    for d in (0, 1):
        for k in (2 * d, 2 * d + 1):
            kv_copy(d, k, half, 2 * half - 1).wait_recv()
        attend(2 * half - 1, d, (z + half) % nz)
    for k in range(4):
        for d in (0, 1):
            kv_copy(d, k, half, 0).wait_send()
    for cp in swap:
        cp.wait_send()

    done = o_ref[...] / l_ref[...]
    for g in range(group):
        att[:, pl.ds(g * HEAD, HEAD)] = done[:, g * 2 * T : (g + 1) * 2 * T].T.astype(BF16)
    c_swap.wait()
    for k in range(2):
        packed[k] = lax.dot_general(
            cbuf[k], att[pl.ds(k * T, T), :], tn, preferred_element_type=F32
        ).astype(BF16)

    mine = pl.ds(pl.multiple_of((x * 2 + c) * QW, HEAD), QW)

    def slots(e, h):
        return pl.ds(pl.multiple_of(e * cap + h * hrow, hrow), hrow)

    def row_half(h):
        return pl.ds(h * hrow, hrow)

    there = ([], [])
    for h in range(2):
        for d, k in sorted(others, key=lambda o: -min(o[0], nx - o[0])):
            e = (x + d) % nx
            there[h].append(
                remote(
                    packed.at[k, slots(e, h), :],
                    arr.at[row_half(h), mine],
                    a_send.at[h, d, k],
                    a_recv.at[h, d, k],
                    {"ctx": z * 2 + (c + k) % 2, "exp": e},
                )
            )
        for cp in there[h]:
            cp.start()
        arr[row_half(h), mine] = packed[0, slots(x, h), :]

    def normalize(h):
        for cp in there[h]:
            cp.wait_recv()
        v32 = arr[row_half(h), :].astype(F32)
        norm = lax.rsqrt(jnp.mean(v32 * v32, axis=-1, keepdims=True) + 1e-05)
        rows[row_half(h), :] = (v32 * norm * gain_ref[...]).astype(BF16)

    def part(ref, pos, k):
        return ref.at[
            pl.ds(pl.multiple_of(pos * cap + (k // 2) * hrow, hrow), hrow), pl.ds((k % 2) * hcol, hcol)
        ]

    def row_copy(d, k, s, pos):
        return remote(
            part(rows, pos, k),
            part(rows, last_pos(d, s), k),
            g_send.at[d, k],
            g_recv.at[d, s - 1, k],
            ahead[d],
        )

    for h in range(2):
        normalize(h)
        for k in (2 * h, 2 * h + 1):
            for d in (0, 1):
                row_copy(d, k, 1, 0).start()
    for cp in w_own:
        cp.wait()
    for cp in w_swap:
        cp.wait()

    M = 4 * cap
    ncols = 4
    ncol = width // ncols

    def activate(src):
        g32 = acc[2 * src]
        hid[src] = (g32 / (1.0 + jnp.exp(-g32)) * acc[2 * src + 1]).T.astype(BF16)

    def project(g, i, cols):
        return lax.dot_general(
            (wg, wu)[i % 2][i // 2, :, cols],
            rows[pl.ds(pl.multiple_of(g * M, M), M), cols],
            nt,
            preferred_element_type=F32,
        )

    def dense(g, i):
        if i < 4:
            acc[i] = project(g, i, pl.ds(0, width))
            if i % 2:
                activate(i // 2)
        else:
            cols = pl.ds((i - 4) * ncol, ncol)
            sums[pl.ds(pl.multiple_of(g * M, M), M), cols] = (
                jnp.dot(hid[0], wd[0, :, cols], preferred_element_type=F32)
                + jnp.dot(hid[1], wd[1, :, cols], preferred_element_type=F32)
            ).astype(BF16)

    pairs = half // 2

    def row_step(s, last):
        for i in range(4):
            for d in (0, 1):
                k = turned(i, d)
                here = last_pos(d, s)
                row_copy(d, k, s, here).wait_recv()
                if not last or k // 2 == d:
                    onward = row_copy(d, k, s + 1, here)
                    onward.wait_send()
                    onward.start()
            yield i

    def row_pair(j, carry):
        for o in range(2):
            for k in row_step(2 * j + 1 + o, False):

                @pl.when(j > 0)
                def _():
                    dense(j - 1, o * 4 + k)

        return carry

    lax.fori_loop(0, pairs - 1, row_pair, 0)
    tail = pairs - 1
    pieces = list(range(8)) if tail > 0 else []
    for i in pieces[:1]:
        dense(tail - 1, i)
    for i in row_step(half - 1, True):
        for piece in (pieces[1:2], pieces[2:], [], [])[i]:
            dense(tail - 1, piece)
    for q in range(2):
        for d in (0, 1):
            row_copy(d, 2 * d + q, half, 2 * half - 1).wait_recv()
        cols = pl.ds(q * hcol, hcol)
        for i in range(4):
            v = project(tail, i, cols)
            acc[i] = v if q == 0 else acc[i] + v
    for src in range(2):
        activate(src)

    def sum_copy(d, k, s):
        pos = 2 * s - s // half if d == 0 else 2 * s - 1
        return remote(
            part(sums, pos, k),
            part(rsb.at[d], s - 1, k),
            r_send.at[d, k],
            r_recv.at[d, s - 1, k],
            ahead[d],
        )

    for q in range(2):
        for i in (4 + 2 * q, 5 + 2 * q):
            dense(tail, i)
        for d in (0, 1):
            sum_copy(d, 2 * d + q, half).start()

    def add_in(d, k, s):
        pos = 2 * s if d == 0 else 2 * s - 1
        sum_copy(d, k, s + 1).wait_recv()
        own = part(sums, pos, k)
        own[...] = (own[...].astype(F32) + part(rsb.at[d], s, k)[...].astype(F32)).astype(BF16)

    def sum_step(t, carry):
        s = half - 1 - t
        for q in range(2):
            for d in (0, 1):
                k = 2 * (1 - d) + q

                @pl.when(t > 0)
                def _():
                    add_in(d, k, s)
                    sum_copy(d, k, s).wait_send()

                sum_copy(d, k, s).start()
        for q in range(2):
            for d in (0, 1):
                k = 2 * d + q
                add_in(d, k, s)
                sum_copy(d, k, s).wait_send()
                sum_copy(d, k, s).start()
        return carry

    lax.fori_loop(0, half - 1, sum_step, 0)

    tw = width // nx
    each = hcol // tw

    def give_back(e, sends):
        cols = pl.ds(e * tw, tw)
        there_x = pl.ds(pl.multiple_of(x * cap, cap), cap)
        step = (e - x + nx) % nx

        @pl.when(e != x)
        def _():
            move = remote(
                comb.at[:, cols],
                ret.at[there_x, :],
                b_send.at[step],
                b_recv.at[step],
                {"ctx": ctx, "exp": e},
            )
            if sends:
                move.start()
            else:
                move.wait_send()

        if sends:

            @pl.when(e == x)
            def _():
                ret[there_x, :] = comb[:, cols]

    for q in range(2):
        for h in range(2):
            k = 2 * h + q
            for d in (0, 1):
                sum_copy(d, k, 1).wait_recv()
            total = part(rows, 0, k)[...].astype(F32) + (
                part(sums, 0, k)[...].astype(F32)
                + part(rsb.at[0], 0, k)[...].astype(F32)
                + part(rsb.at[1], 0, k)[...].astype(F32)
            )
            part(comb, 0, k)[...] = total.astype(BF16)
        for e in range(q * each, (q + 1) * each):
            give_back(e, True)
    for cp in there[0] + there[1]:
        cp.wait_send()
    for k in range(4):
        for d in (0, 1):
            row_copy(d, k, half, 0).wait_send()
            sum_copy(d, k, 1).wait_send()
    for e in range(nx):
        give_back(e, False)
    for d in range(1, nx):
        e = (x + nx - d) % nx
        spot = pl.ds(pl.multiple_of(e * cap, cap), cap)
        remote(comb.at[:, pl.ds(0, tw)], ret.at[spot, :], b_send.at[d], b_recv.at[d], {"ctx": ctx, "exp": e}).wait_recv()
    out_ref[...] = jnp.dot(cbuf[0], ret[...], preferred_element_type=F32).astype(BF16)


def on_device(
    nz,
    nx,
    queries,
    new_keys,
    new_values,
    cache_keys,
    cache_values,
    offset,
    token_ids,
    expert_table,
    norm_gain,
    w_gate,
    w_up,
    w_down,
):
    T = queries.shape[0]
    cap = T // 2
    width = norm_gain.shape[0]
    QW = queries.shape[1] // 2
    span = cache_keys.shape[0] + new_keys.shape[0]
    ff = w_gate.shape[2]
    half = nz // 2
    lanes = 2 * T * (QW // HEAD)
    hbm = pl.BlockSpec(memory_space=pltpu.HBM)
    vmem = pl.BlockSpec(memory_space=pltpu.VMEM)
    smem = pl.BlockSpec(memory_space=pltpu.SMEM)
    dma = pltpu.SemaphoreType.DMA
    return pl.pallas_call(
        functools.partial(layer_kernel, nz, nx),
        out_shape=jax.ShapeDtypeStruct(queries.shape, BF16),
        in_specs=[vmem, smem] + [hbm] * 10,
        out_specs=vmem,
        scratch_shapes=[
            pltpu.VMEM((nz, 2, span, HEAD), BF16),
            pltpu.VMEM((nz, 2, span, HEAD), BF16),
            pltpu.VMEM((2, T, QW), BF16),
            pltpu.VMEM((lanes, HEAD), BF16),
            pltpu.VMEM((2, T, nx * cap), BF16),
            pltpu.VMEM((expert_table.shape[0] // HEAD, HEAD), jnp.int32),
            pltpu.VMEM((T, HEAD), jnp.int32),
            pltpu.VMEM((1, width), F32),
            pltpu.VMEM((1, lanes), jnp.int32),
            pltpu.VMEM((1, lanes), F32),
            pltpu.VMEM((1, lanes), F32),
            pltpu.VMEM((HEAD, lanes), F32),
            pltpu.VMEM((2 * T, QW), BF16),
            pltpu.VMEM((2, nx * cap, QW), BF16),
            pltpu.VMEM((cap, width), BF16),
            pltpu.VMEM((nz * cap, width), BF16),
            pltpu.VMEM((nz * cap, width), BF16),
            pltpu.VMEM((2, half * cap, width), BF16),
            pltpu.VMEM((4, ff, 4 * cap), F32),
            pltpu.VMEM((2, 4 * cap, ff), BF16),
            pltpu.VMEM((cap, width), BF16),
            pltpu.VMEM((nx * cap, width // nx), BF16),
            pltpu.VMEM((2, ff, width), BF16),
            pltpu.VMEM((2, ff, width), BF16),
            pltpu.VMEM((2,) + w_down.shape[1:], BF16),
            dma((7,)),
            dma((6,)),
            dma((6,)),
            dma((3,)),
            dma((3,)),
            dma((3,)),
            dma((2, 4)),
            dma((2, half, 4)),
            dma((2, nx, 2)),
            dma((2, nx, 2)),
            dma((2, 4)),
            dma((2, half, 4)),
            dma((2, 4)),
            dma((2, half, 4)),
            dma((nx,)),
            dma((nx,)),
        ],
        compiler_params=pltpu.CompilerParams(
            collective_id=0, has_side_effects=True, vmem_limit_bytes=VMEM_LIMIT
        ),
    )(
        offset.reshape(1, 1),
        token_ids,
        queries,
        new_keys,
        new_values,
        cache_keys,
        cache_values,
        expert_table.reshape(-1, HEAD),
        norm_gain.reshape(1, width),
        jnp.swapaxes(w_gate, 1, 2),
        jnp.swapaxes(w_up, 1, 2),
        w_down,
    )


def solution(mesh):
    split = ("group", "ctx")
    tokens = P(split, "exp")
    placed = (
        tokens,
        tokens,
        tokens,
        tokens,
        tokens,
        P("group"),
        P(split),
        P("group"),
        P(),
        P("exp", None, "ctx"),
        P("exp", None, "ctx"),
        P("exp", "ctx", None),
    )
    return jax.shard_map(
        functools.partial(on_device, mesh.shape["ctx"] // 2, mesh.shape["exp"]),
        mesh=mesh,
        in_specs=placed,
        out_specs=tokens,
        check_vma=False,
    )
```
